512 devices in a mesh: seq: 64 (over y_hi, x, z), bat: 8 (over y_lo, core).
Axes of the slice: x: 4, y: 8 (y_hi: 2, y_lo: 4; y = y_hi * 4 + y_lo), z: 8, core: 2. Of those that a mesh axis runs over, the one named last changes fastest.
Arguments:
- tokens: bfloat16 [8, 65536, 256], P('bat', 'seq'), may hold values from -6 to 6
- filter_spectrum: bfloat16 [2, 256, 256, 256], P(None, 'seq', None, 'bat'), may hold values from -6 to 6
- skip_gain: float32 [256], replicated, may hold values from 0.5 to 1.5
Outputs:
- mixed: bfloat16 [8, 65536, 256], P('bat', 'seq')
The draws below stay inside these ranges and needn't reach their ends.
All inputs are finite; a program needn't handle non-finite values.
Results may differ from the reference program's by a relative error of at most 0.012.
Values may be sent and summed in bfloat16 or wider, within the bound.
No kernel may reach another device: no remote copies, remote signals or barrier semaphores. Data moves between devices by JAX's collectives and lax.ppermute only.
A program may use at most 64 MiB of HBM per device.

```python
import math
import jax
import jax.numpy as jnp
from jax import lax

C = 256
N1 = 256
N2 = 256
BATCH = 8
LENGTH = 65536


def level_of(own_key, shape, pieces, least, largest):
    def one(dim, parts):
        steps = jax.random.uniform(jax.random.fold_in(jax.random.fold_in(own_key, 6), dim), (parts,), jnp.float32, least / len(pieces), largest / len(pieces))
        return jnp.repeat(jnp.exp(steps), shape[dim] // parts).reshape((-1,) + (1,) * (len(shape) - dim - 1))

    gain = one(*pieces[0])
    for cut in pieces[1:]:
        gain = gain * one(*cut)
    return gain


def noise(key, shape, scale, most, shards=(), kind=jnp.bfloat16):
    array = jax.random.normal(key, shape, jnp.float32) * scale
    if len(shards) > 0:
        array = level_of(key, shape, shards, -0.22, 0.18) * array
    return jnp.clip(array, min=-most, max=most).astype(kind)


def setup_inputs(seed: int = 0) -> dict:
    key_of = jax.random.split(jax.random.key(seed), 4)
    return {
        "tokens": noise(key_of[0], (BATCH, LENGTH, C), 1.0, 6.0, ((0, 8), (1, 64))),
        "filter_spectrum": noise(key_of[1], (2, N1, N2, C), 1.0, 6.0, ((1, 64), (3, 8))),
        "skip_gain": jnp.clip(jax.random.uniform(key_of[2], (C,), jnp.float32, 0.5, 1.5), 0.5, 1.5),
    }


def cos_sin(points):
    steps_range = jnp.arange(points, dtype=jnp.int32)
    index_grid = (steps_range[:, None] * steps_range[None, :]) % points
    phase_angle = index_grid.astype(jnp.float32) * (2.0 * math.pi / points)
    return jnp.cos(phase_angle), jnp.sin(phase_angle)


def real_table(points):
    cosine, sine_vals = cos_sin(points)
    return jnp.stack([cosine, -sine_vals], axis=1).astype(jnp.bfloat16)


def complex_table(points, signum, factor):
    cosine, sine_vals = cos_sin(points)
    top_rows = jnp.stack([cosine, signum * sine_vals], axis=1)
    low_rows = jnp.stack([-signum * sine_vals, cosine], axis=1)
    return (jnp.stack([top_rows, low_rows], axis=0) * factor).astype(jnp.bfloat16)


def final_table(points):
    cosine, sine_vals = cos_sin(points)
    return (jnp.stack([cosine, -sine_vals], axis=0) / points).astype(jnp.bfloat16)


def twiddle_phase(first_rows, second_rows, period):
    index_grid = (first_rows[:, None] * second_rows[None, :]) % period
    phase_angle = index_grid.astype(jnp.float32) * (2.0 * math.pi / period)
    return jnp.cos(phase_angle)[..., None], jnp.sin(phase_angle)[..., None]


def round_half(values):
    return lax.optimization_barrier(values.astype(jnp.bfloat16)).astype(jnp.float32)


def reference(tokens, filter_spectrum, skip_gain):
    period = N1 * N2
    forward_rows = real_table(N1).astype(jnp.float32)
    forward_cols = complex_table(N2, -1.0, 1.0).astype(jnp.float32)
    inverse_cols = complex_table(N2, 1.0, 1.0 / N2).astype(jnp.float32)
    inverse_rows = final_table(N1).astype(jnp.float32)
    cos_tw, sin_tw = twiddle_phase(jnp.arange(N1, dtype=jnp.int32), jnp.arange(N2, dtype=jnp.int32), period)
    filters_f32 = filter_spectrum.astype(jnp.float32)

    def one_sequence(sequence):
        columns = sequence.reshape(N1, N2, C).astype(jnp.float32)
        first_section = jnp.einsum("nmc,nsk->skmc", columns, forward_rows)
        real_part = first_section[0] * cos_tw + first_section[1] * sin_tw
        imag_part = first_section[1] * cos_tw - first_section[0] * sin_tw
        turned = round_half(jnp.stack([real_part, imag_part]))
        spectrum = round_half(jnp.einsum("rknc,rnsj->skjc", turned, forward_cols))
        prod_real = spectrum[0] * filters_f32[0] - spectrum[1] * filters_f32[1]
        prod_imag = spectrum[0] * filters_f32[1] + spectrum[1] * filters_f32[0]
        product = round_half(jnp.stack([prod_real, prod_imag]))
        back_section = jnp.einsum("rkjc,rjsn->sknc", product, inverse_cols)
        real_back = back_section[0] * cos_tw - back_section[1] * sin_tw
        imag_back = back_section[0] * sin_tw + back_section[1] * cos_tw
        turned_back = round_half(jnp.stack([real_back, imag_back]))
        filtered = jnp.einsum("rknc,rkm->mnc", turned_back, inverse_rows)
        result = filtered + skip_gain * columns
        return result.astype(jnp.bfloat16).reshape(N1 * N2, C)

    return lax.map(one_sequence, tokens)
```

```python
import math

import jax
import jax.numpy as jnp
from jax import lax
from jax.experimental import pallas as pl
from jax.experimental.pallas import tpu as pltpu
from jax.sharding import Mesh
from jax.sharding import PartitionSpec as P

N1 = 256
N2 = 256
HALF = 128


def cos_sin(points):
    steps_range = jnp.arange(points, dtype=jnp.int32)
    index_grid = steps_range[:, None] * steps_range[None, :] % points
    phase_angle = index_grid.astype(jnp.float32) * (2.0 * math.pi / points)
    return (jnp.cos(phase_angle), jnp.sin(phase_angle))


def twiddle_phase():
    period = N1 * N2
    index_grid = jnp.arange(N1, dtype=jnp.int32)[:, None] * jnp.arange(N2, dtype=jnp.int32)[None, :] % period
    phase_angle = index_grid.astype(jnp.float32) * (2.0 * math.pi / period)
    return (jnp.cos(phase_angle), jnp.sin(phase_angle))


def spread_rows(table):
    eye = jnp.eye(2, dtype=table.dtype)
    wide = eye[:, None, None, :] * table[None, :, :, None]
    return wide.reshape(2 * N1, 2 * N1)


def tables():
    cosine, sine = cos_sin(N1)
    c16, s16 = cosine.astype(jnp.bfloat16), sine.astype(jnp.bfloat16)
    ci = (cosine / N1).astype(jnp.bfloat16)
    si = (sine / N1).astype(jnp.bfloat16)
    first = jnp.concatenate([spread_rows(c16), spread_rows(-s16)], axis=0)
    second = jnp.concatenate(
        [jnp.concatenate([c16, -s16], axis=1), jnp.concatenate([s16, c16], axis=1)], axis=0
    )
    third = jnp.concatenate(
        [jnp.concatenate([ci, si], axis=1), jnp.concatenate([-si, ci], axis=1)], axis=0
    )
    fourth = jnp.concatenate([spread_rows(ci).T, spread_rows(-si).T], axis=1)
    return first, second, third, fourth


def row_order():
    want = jnp.arange(2 * N1, dtype=jnp.int32)
    part, k1 = want // N1, want % N1
    source = (k1 // 4) * 8 + part * 4 + k1 % 4
    return (source[:, None] == jnp.arange(2 * N1, dtype=jnp.int32)[None, :]).astype(jnp.bfloat16)


def dot(a, b):
    return jnp.dot(a, b, preferred_element_type=jnp.float32)


def convolve(gain, u, filt, order, first, second, third, fourth, cos_tw, sin_tw, out):
    weights = dot(order[...], filt[...])
    wr, wi = weights[:N1], weights[N1:]
    c, s = cos_tw[...], sin_tw[...]
    batches = u.shape[0]
    section = dot(first[...], jnp.concatenate([u[b] for b in range(batches)], axis=1))
    for b in range(batches):
        lanes = slice(b * HALF, (b + 1) * HALF)
        piece = section[:, lanes]
        re = jnp.concatenate([piece[:N1], piece[N1 : 2 * N1]], axis=1)
        im = jnp.concatenate([piece[2 * N1 : 3 * N1], piece[3 * N1 :]], axis=1)
        turned = jnp.concatenate([re * c + im * s, im * c - re * s], axis=1).astype(jnp.bfloat16)
        spectrum = dot(turned, second[...])
        sr, si = spectrum[:, :N2], spectrum[:, N2:]
        product = jnp.concatenate([sr * wr - si * wi, sr * wi + si * wr], axis=1).astype(jnp.bfloat16)
        back = dot(product, third[...])
        br, bi = back[:, :N2], back[:, N2:]
        tr = (br * c - bi * s).astype(jnp.bfloat16)
        ti = (br * s + bi * c).astype(jnp.bfloat16)
        rows = jnp.concatenate([tr[:, :HALF], tr[:, HALF:], ti[:, :HALF], ti[:, HALF:]], axis=0)
        filtered = dot(fourth[...], rows)
        out[b] = (filtered + gain[0] * u[b].astype(jnp.float32)).astype(jnp.bfloat16)


def body(tokens, filter_spectrum, skip_gain):
    channels = tokens.shape[-1]
    channel = lax.axis_index("ylo") * lax.axis_size("seq") + lax.axis_index("seq")
    laid_out = tokens.reshape(8, HALF, channels).transpose(2, 0, 1)
    u = lax.all_to_all(laid_out, ("ylo", "seq"), split_axis=0, concat_axis=0, tiled=True)
    u = u.reshape(4, 2 * N1, HALF)
    mine = filter_spectrum.transpose(3, 0, 1, 2)
    both = lax.all_gather(mine, "core", axis=0, tiled=True)
    both = both.reshape(both.shape[0], 8, N2)
    filt = lax.all_to_all(both, "seq", split_axis=0, concat_axis=0, tiled=True)
    filt = filt.reshape(2 * N1, N2)
    gain = lax.dynamic_slice(skip_gain, (channel,), (1,))
    first, second, third, fourth = tables()
    cos_tw, sin_tw = twiddle_phase()
    vmem = pl.BlockSpec(memory_space=pltpu.VMEM)
    mixed = pl.pallas_call(
        convolve,
        out_shape=jax.ShapeDtypeStruct((4, 2 * N1, HALF), jnp.bfloat16),
        in_specs=[pl.BlockSpec(memory_space=pltpu.SMEM)] + [vmem] * 9,
        out_specs=vmem,
    )(gain, u, filt, row_order(), first, second, third, fourth, cos_tw, sin_tw)
    mixed = mixed.reshape(4 * 64, 8, HALF)
    back = lax.all_to_all(mixed, ("ylo", "seq"), split_axis=0, concat_axis=0, tiled=True)
    return back.transpose(1, 2, 0).reshape(1, 8 * HALF, channels)


def solution(mesh):
    names = mesh.axis_names
    assert names == ("seq", "bat")
    split = Mesh(mesh.devices.reshape(64, 4, 2), ("seq", "ylo", "core"))
    bat = ("ylo", "core")
    placed = (P(bat, "seq", None), P(None, "seq", None, bat), P())
    return jax.shard_map(
        body, mesh=split, in_specs=placed, out_specs=P(bat, "seq", None), check_vma=False
    )
```

```python
import math

import jax
import jax.numpy as jnp
from jax import lax
from jax.experimental import pallas as pl
from jax.experimental.pallas import tpu as pltpu
from jax.sharding import Mesh
from jax.sharding import PartitionSpec as P

N1 = 256
N2 = 256
HALF = 128
TOKEN_GROUP = ("ylo", "yh", "xz")


def cos_sin(points):
    steps_range = jnp.arange(points, dtype=jnp.int32)
    index_grid = steps_range[:, None] * steps_range[None, :] % points
    phase_angle = index_grid.astype(jnp.float32) * (2.0 * math.pi / points)
    return (jnp.cos(phase_angle), jnp.sin(phase_angle))


def twiddle_phase():
    period = N1 * N2
    index_grid = jnp.arange(N1, dtype=jnp.int32)[:, None] * jnp.arange(N2, dtype=jnp.int32)[None, :] % period
    phase_angle = index_grid.astype(jnp.float32) * (2.0 * math.pi / period)
    return (jnp.cos(phase_angle), jnp.sin(phase_angle))


def spread_rows(table):
    eye = jnp.eye(2, dtype=table.dtype)
    wide = eye[:, None, None, :] * table[None, :, :, None]
    return wide.reshape(2 * N1, 2 * N1)


def tables():
    cosine, sine = cos_sin(N1)
    c16, s16 = cosine.astype(jnp.bfloat16), sine.astype(jnp.bfloat16)
    ci = (cosine / N1).astype(jnp.bfloat16)
    si = (sine / N1).astype(jnp.bfloat16)
    first = jnp.concatenate([spread_rows(c16), spread_rows(-s16)], axis=0)
    second = jnp.concatenate(
        [jnp.concatenate([c16, -s16], axis=1), jnp.concatenate([s16, c16], axis=1)], axis=0
    )
    third = jnp.concatenate(
        [jnp.concatenate([ci, si], axis=1), jnp.concatenate([-si, ci], axis=1)], axis=0
    )
    fourth = jnp.concatenate([spread_rows(ci).T, spread_rows(-si).T], axis=1)
    return first, second, third, fourth


def row_order():
    want = jnp.arange(2 * N1, dtype=jnp.int32)
    part, k1 = want // N1, want % N1
    source = (k1 // 4) * 8 + part * 4 + k1 % 4
    return (source[:, None] == jnp.arange(2 * N1, dtype=jnp.int32)[None, :]).astype(jnp.bfloat16)


def dot(a, b):
    return jnp.dot(a, b, preferred_element_type=jnp.float32)


def convolve(gain, u, filt, order, first, second, third, fourth, cos_tw, sin_tw, out):
    weights = dot(order[...], filt[...])
    wr, wi = weights[:N1], weights[N1:]
    c, s = cos_tw[...], sin_tw[...]
    batches = u.shape[0]
    section = dot(first[...], jnp.concatenate([u[b] for b in range(batches)], axis=1))
    for b in range(batches):
        lanes = slice(b * HALF, (b + 1) * HALF)
        piece = section[:, lanes]
        re = jnp.concatenate([piece[:N1], piece[N1 : 2 * N1]], axis=1)
        im = jnp.concatenate([piece[2 * N1 : 3 * N1], piece[3 * N1 :]], axis=1)
        turned = jnp.concatenate([re * c + im * s, im * c - re * s], axis=1).astype(jnp.bfloat16)
        spectrum = dot(turned, second[...])
        sr, si = spectrum[:, :N2], spectrum[:, N2:]
        product = jnp.concatenate([sr * wr - si * wi, sr * wi + si * wr], axis=1).astype(jnp.bfloat16)
        back = dot(product, third[...])
        br, bi = back[:, :N2], back[:, N2:]
        tr = (br * c - bi * s).astype(jnp.bfloat16)
        ti = (br * s + bi * c).astype(jnp.bfloat16)
        rows = jnp.concatenate([tr[:, :HALF], tr[:, HALF:], ti[:, :HALF], ti[:, HALF:]], axis=0)
        filtered = dot(fourth[...], rows)
        out[b] = (filtered + gain[0] * u[b].astype(jnp.float32)).astype(jnp.bfloat16)


def body(tokens, filter_spectrum, skip_gain):
    channels = tokens.shape[-1]
    channel = lax.axis_index(("ylo", "yh", "xz"))
    laid_out = tokens.reshape(8, HALF, channels).transpose(2, 0, 1)
    with jax.named_scope("tok"):
        u = lax.all_to_all(laid_out, TOKEN_GROUP, split_axis=0, concat_axis=0, tiled=True)
    u = u.reshape(4, 2 * N1, HALF)
    mine = filter_spectrum.transpose(3, 0, 1, 2).reshape(32, 8, N2)
    with jax.named_scope("flt"):
        mine = lax.all_to_all(mine, "xz", split_axis=0, concat_axis=0, tiled=True)
        with jax.named_scope("turn"):
            mine = lax.ppermute(mine, ("yh", "core"), [(0, 0), (1, 2), (2, 1), (3, 3)])
        with jax.named_scope("pair"):
            filt = lax.all_gather(mine, "core", axis=0, tiled=True)
    filt = filt.reshape(2 * N1, N2)
    gain = lax.dynamic_slice(skip_gain, (channel,), (1,))
    first, second, third, fourth = tables()
    cos_tw, sin_tw = twiddle_phase()
    vmem = pl.BlockSpec(memory_space=pltpu.VMEM)
    mixed = pl.pallas_call(
        convolve,
        out_shape=jax.ShapeDtypeStruct((4, 2 * N1, HALF), jnp.bfloat16),
        in_specs=[pl.BlockSpec(memory_space=pltpu.SMEM)] + [vmem] * 9,
        out_specs=vmem,
    )(gain, u, filt, row_order(), first, second, third, fourth, cos_tw, sin_tw)
    mixed = mixed.reshape(4 * 64, 8, HALF)
    back = lax.all_to_all(mixed, TOKEN_GROUP, split_axis=0, concat_axis=0, tiled=True)
    return back.transpose(1, 2, 0).reshape(1, 8 * HALF, channels)


def solution(mesh):
    names = mesh.axis_names
    assert names == ("seq", "bat")
    split = Mesh(mesh.devices.reshape(2, 32, 4, 2), ("yh", "xz", "ylo", "core"))
    bat, seq = ("ylo", "core"), ("yh", "xz")
    placed = (P(bat, seq, None), P(None, seq, None, bat), P())
    return jax.shard_map(
        body, mesh=split, in_specs=placed, out_specs=P(bat, seq, None), check_vma=False
    )
```

```python
import math

import jax
import jax.numpy as jnp
from jax import lax
from jax.experimental import pallas as pl
from jax.experimental.pallas import tpu as pltpu
from jax.sharding import Mesh
from jax.sharding import PartitionSpec as P


N1 = 256
N2 = 256
HALF = 128
TOKEN_GROUP = ("ylo", "yh", "xz")
VMEM = pl.BlockSpec(memory_space=pltpu.VMEM)
HBM = pl.BlockSpec(memory_space=pltpu.HBM)
KERNEL = pltpu.CompilerParams(vmem_limit_bytes=24 * 1024 * 1024)


def grid_of(shape, dim):
    return lax.broadcasted_iota(jnp.int32, shape, dim)


def make_tables(first, second, fourth, cos_tw, sin_tw, order):
    def cos_sin(period):
        square = (N1, N2)
        index_grid = grid_of(square, 0) * grid_of(square, 1) % period
        angle = index_grid.astype(jnp.float32) * (2.0 * math.pi / period)
        return jnp.cos(angle), jnp.sin(angle)

    c, s = cos_sin(N1)
    c16, s16, n16 = c.astype(jnp.bfloat16), s.astype(jnp.bfloat16), (-s).astype(jnp.bfloat16)
    second[:N2, :N2] = c16
    second[:N2, N2:] = n16
    second[N2:, :N2] = s16
    second[N2:, N2:] = c16
    tall, wide = jnp.concatenate([c16, n16], axis=0), jnp.concatenate([c16, n16], axis=1)
    for half in range(2):
        spread = (N1, 2 * N1)
        pick = jnp.where(grid_of(spread, 1) == 2 * grid_of(spread, 0) + half, 1.0, 0.0).astype(jnp.bfloat16)
        block = dot(tall, pick).astype(jnp.bfloat16)
        first[half * N1 : (half + 1) * N1, :] = block[:N1]
        first[(2 + half) * N1 : (3 + half) * N1, :] = block[N1:]
        spread = (2 * N1, N1)
        pick = jnp.where(grid_of(spread, 0) == 2 * grid_of(spread, 1) + half, 1.0, 0.0).astype(jnp.bfloat16)
        block = dot(pick, wide).astype(jnp.bfloat16)
        fourth[:, half * N1 : (half + 1) * N1] = block[:, :N1]
        fourth[:, (2 + half) * N1 : (3 + half) * N1] = block[:, N1:]
    c, s = cos_sin(N1 * N2)
    cos_tw[...] = c
    sin_tw[...] = s
    full = (2 * N1, 2 * N1)
    want = grid_of(full, 0)
    part, k1 = want // N1, want % N1
    source = (k1 // 4) * 8 + part * 4 + k1 % 4
    order[...] = jnp.where(source == grid_of(full, 1), 1.0, 0.0).astype(jnp.bfloat16)


def dot(a, b):
    return jnp.dot(a, b, preferred_element_type=jnp.float32)


def convolve(gain, u, filt, first, fourth, second_hbm, cos_hbm, sin_hbm, order_hbm, out, second, cos_tw, sin_tw, order, arrived):
    late = ((cos_hbm, cos_tw), (sin_hbm, sin_tw), (second_hbm, second), (order_hbm, order))
    copies = [pltpu.make_async_copy(far, near, arrived.at[i]) for i, (far, near) in enumerate(late)]
    for copy in copies:
        copy.start()
    batches = u.shape[0]
    section = dot(first[...], jnp.concatenate([u[b] for b in range(batches)], axis=1))
    for copy in copies:
        copy.wait()
    c, s = cos_tw[...], sin_tw[...]
    weights = dot(order[...], filt[...])
    wr, wi = weights[:N1], weights[N1:]
    for b in range(batches):
        lanes = slice(b * HALF, (b + 1) * HALF)
        piece = section[:, lanes]
        re = jnp.concatenate([piece[:N1], piece[N1 : 2 * N1]], axis=1)
        im = jnp.concatenate([piece[2 * N1 : 3 * N1], piece[3 * N1 :]], axis=1)
        turned = jnp.concatenate([re * c + im * s, im * c - re * s], axis=1).astype(jnp.bfloat16)
        spectrum = dot(turned, second[...])
        sr, si = spectrum[:, :N2], spectrum[:, N2:]
        product = jnp.concatenate([sr * wr - si * wi, -(sr * wi) - si * wr], axis=1).astype(jnp.bfloat16)
        back = dot(product, second[...])
        br, nbi = back[:, :N2], back[:, N2:]
        tr = (br * c + nbi * s).astype(jnp.bfloat16)
        ti = (br * s - nbi * c).astype(jnp.bfloat16)
        rows = jnp.concatenate([tr[:, :HALF], tr[:, HALF:], ti[:, :HALF], ti[:, HALF:]], axis=0)
        filtered = dot(fourth[...], rows) * (1.0 / (N1 * N2))
        out[b] = (filtered + gain[0] * u[b].astype(jnp.float32)).astype(jnp.bfloat16)


def layer(tokens, filter_spectrum, skip_gain):
    channels = tokens.shape[-1]
    channel = lax.axis_index(TOKEN_GROUP)
    laid_out = tokens.reshape(8, HALF, channels).transpose(2, 0, 1)
    u = lax.all_to_all(laid_out, TOKEN_GROUP, split_axis=0, concat_axis=0, tiled=True)
    u = u.reshape(4, 2 * N1, HALF)
    mine = filter_spectrum.transpose(3, 0, 1, 2).reshape(32, 8, N2)
    mine = lax.all_to_all(mine, "xz", split_axis=0, concat_axis=0, tiled=True)
    mine = lax.ppermute(mine, ("yh", "core"), [(0, 0), (1, 2), (2, 1), (3, 3)])
    filt = lax.all_gather(mine, "core", axis=0, tiled=True)
    filt = filt.reshape(2 * N1, N2)
    gain = lax.dynamic_slice(skip_gain, (channel,), (1,))
    first, second, fourth, cos_tw, sin_tw, order = pl.pallas_call(
        make_tables,
        out_shape=[
            jax.ShapeDtypeStruct((4 * N1, 2 * N1), jnp.bfloat16),
            pltpu.HBM((2 * N2, 2 * N2), jnp.bfloat16),
            jax.ShapeDtypeStruct((2 * N1, 4 * N1), jnp.bfloat16),
            pltpu.HBM((N1, N2), jnp.float32),
            pltpu.HBM((N1, N2), jnp.float32),
            pltpu.HBM((2 * N1, 2 * N1), jnp.bfloat16),
        ],
        out_specs=[VMEM, VMEM, VMEM, VMEM, VMEM, VMEM],
        compiler_params=KERNEL,
    )()
    second, cos_tw, sin_tw, order = (
        pltpu.with_memory_space_constraint(table, pltpu.HBM) for table in (second, cos_tw, sin_tw, order)
    )
    mixed = pl.pallas_call(
        convolve,
        out_shape=jax.ShapeDtypeStruct((4, 2 * N1, HALF), jnp.bfloat16),
        in_specs=[pl.BlockSpec(memory_space=pltpu.SMEM)] + [VMEM] * 4 + [HBM] * 4,
        out_specs=VMEM,
        scratch_shapes=[
            pltpu.VMEM((2 * N2, 2 * N2), jnp.bfloat16),
            pltpu.VMEM((N1, N2), jnp.float32),
            pltpu.VMEM((N1, N2), jnp.float32),
            pltpu.VMEM((2 * N1, 2 * N1), jnp.bfloat16),
            pltpu.SemaphoreType.DMA((4,)),
        ],
        compiler_params=KERNEL,
    )(gain, u, filt, first, fourth, second, cos_tw, sin_tw, order)
    mixed = mixed.reshape(4 * 64, 8, HALF)
    back = lax.all_to_all(mixed, TOKEN_GROUP, split_axis=0, concat_axis=0, tiled=True)
    return back.transpose(1, 2, 0).reshape(1, 8 * HALF, channels)


def solution(mesh):
    split = Mesh(mesh.devices.reshape(2, 32, 4, 2), ("yh", "xz", "ylo", "core"))
    bat, seq = ("ylo", "core"), ("yh", "xz")
    placed = (P(bat, seq, None), P(None, seq, None, bat), P())
    return jax.shard_map(layer, mesh=split, in_specs=placed, out_specs=P(bat, seq, None), check_vma=False)
```

```python
import math

import jax
import jax.numpy as jnp
import numpy as np
from jax import lax
from jax.experimental import pallas as pl
from jax.experimental.pallas import tpu as pltpu
from jax.sharding import Mesh
from jax.sharding import PartitionSpec as P


N1 = 256
N2 = 256
HALF = 128
EVERY = ("yh", "xz", "ylo", "core")


def home(ylo, core):
    return (ylo + 2 + 4 * core) % 8


TOKEN_GROUPS = [
    [
        ((home(ylo, block) // 4 * 32 + xz) * 4 + home(ylo, block) % 4) * 2 + core
        for ylo in range(4)
        for block in range(2)
        for xz in range(32)
    ]
    for core in range(2)
]
MEET = [
    ((yh * 4 + ylo) * 2 + core, home(ylo, core) * 2 + yh)
    for yh in range(2)
    for ylo in range(4)
    for core in range(2)
]
VMEM = pl.BlockSpec(memory_space=pltpu.VMEM)
HBM = pl.BlockSpec(memory_space=pltpu.HBM)
KERNEL = pltpu.CompilerParams(vmem_limit_bytes=24 * 1024 * 1024)


def grid_of(shape, dim):
    return lax.broadcasted_iota(jnp.int32, shape, dim)


def cos_sin(period):
    steps = np.arange(N1)
    angle = (steps[:, None] * steps[None, :] % period) * (2.0 * math.pi / period)
    return np.cos(angle).astype(np.float32), np.sin(angle).astype(np.float32)


def complex_table():
    c, s = cos_sin(N2)
    return np.block([[c, -s], [s, c]]).astype(jnp.bfloat16)


def make_tables(second, first, fourth, order):
    c16, n16 = second[:N2, :N2], second[:N2, N2:]
    tall, wide = jnp.concatenate([c16, n16], axis=0), jnp.concatenate([c16, n16], axis=1)
    for half in range(2):
        spread = (N1, 2 * N1)
        pick = jnp.where(grid_of(spread, 1) == 2 * grid_of(spread, 0) + half, 1.0, 0.0).astype(jnp.bfloat16)
        block = dot(tall, pick).astype(jnp.bfloat16)
        first[half * N1 : (half + 1) * N1, :] = block[:N1]
        first[(2 + half) * N1 : (3 + half) * N1, :] = block[N1:]
        spread = (2 * N1, N1)
        pick = jnp.where(grid_of(spread, 0) == 2 * grid_of(spread, 1) + half, 1.0, 0.0).astype(jnp.bfloat16)
        block = dot(pick, wide).astype(jnp.bfloat16)
        fourth[:, half * N1 : (half + 1) * N1] = block[:, :N1]
        fourth[:, (2 + half) * N1 : (3 + half) * N1] = block[:, N1:]
    full = (HALF, HALF)
    want = grid_of(full, 0)
    source = (want // 4 % 16) * 8 + (want // 64) * 4 + want % 4
    order[...] = jnp.where(source == grid_of(full, 1), 1.0, 0.0).astype(jnp.bfloat16)


def dot(a, b):
    return jnp.dot(a, b, preferred_element_type=jnp.float32)


def convolve(gains_hbm, u, filt, order, first, second, cos_tw, sin_tw, fourth_hbm, out, gains, fourth, arrived):
    copies = (
        pltpu.make_async_copy(gains_hbm, gains, arrived.at[0]),
        pltpu.make_async_copy(fourth_hbm, fourth, arrived.at[1]),
    )
    for copy in copies:
        copy.start()
    block = (lax.axis_index("yh") * 4 + lax.axis_index("ylo") + 6) % 8
    channel = (block % 4) * 64 + (block // 4) * 32 + lax.axis_index("xz")
    batches = u.shape[0]
    section = dot(first[...], jnp.concatenate([u[b] for b in range(batches)], axis=1))
    blocks = [dot(order[...], filt[i * HALF : (i + 1) * HALF]) for i in range(4)]
    wr = jnp.concatenate([block[:64] for block in blocks], axis=0)
    wi = jnp.concatenate([block[64:] for block in blocks], axis=0)
    c, s = cos_tw[...], sin_tw[...]
    for first_of_two in range(0, batches, 2):
        two = []
        for b in (first_of_two, first_of_two + 1):
            piece = section[:, b * HALF : (b + 1) * HALF]
            re = jnp.concatenate([piece[:N1], piece[N1 : 2 * N1]], axis=1)
            im = jnp.concatenate([piece[2 * N1 : 3 * N1], piece[3 * N1 :]], axis=1)
            turned = jnp.concatenate([re * c + im * s, im * c - re * s], axis=1).astype(jnp.bfloat16)
            spectrum = dot(turned, second[...])
            sr, si = spectrum[:, :N2], spectrum[:, N2:]
            product = jnp.concatenate([sr * wr - si * wi, -(sr * wi) - si * wr], axis=1).astype(jnp.bfloat16)
            back = dot(product, second[...])
            br, nbi = back[:, :N2], back[:, N2:]
            tr = (br * c + nbi * s).astype(jnp.bfloat16)
            ti = (br * s - nbi * c).astype(jnp.bfloat16)
            two.append(jnp.concatenate([tr[:, :HALF], tr[:, HALF:], ti[:, :HALF], ti[:, HALF:]], axis=0))
        if first_of_two == 0:
            for copy in copies:
                copy.wait()
        filtered = dot(fourth[...], jnp.concatenate(two, axis=1)) * (1.0 / (N1 * N2))
        for i in range(2):
            b = first_of_two + i
            skip = gains[channel] * u[b].astype(jnp.float32)
            out[b] = (filtered[:, i * HALF : (i + 1) * HALF] + skip).astype(jnp.bfloat16)


def exchange(chunks):
    return lax.all_to_all(
        chunks, EVERY, split_axis=0, concat_axis=0, tiled=True, axis_index_groups=TOKEN_GROUPS
    )


def layer(tokens, filter_spectrum, skip_gain):
    channels = tokens.shape[-1]
    mine = filter_spectrum.transpose(3, 0, 1, 2).reshape(32, 8, N2)
    mine = lax.all_to_all(mine, "xz", split_axis=0, concat_axis=0, tiled=True)
    laid_out = tokens.reshape(8, HALF, channels).transpose(2, 0, 1)
    u = exchange(laid_out)
    u = u.reshape(4, 2 * N1, HALF)
    mine = lax.ppermute(mine, ("yh", "ylo", "core"), MEET)
    filt = lax.all_gather(mine, "core", axis=0, tiled=True)
    filt = filt.reshape(2 * N1, N2)
    second = jnp.asarray(complex_table())
    cos_tw, sin_tw = (jnp.asarray(table) for table in cos_sin(N1 * N2))
    first, fourth, order = pl.pallas_call(
        make_tables,
        out_shape=[
            jax.ShapeDtypeStruct((4 * N1, 2 * N1), jnp.bfloat16),
            pltpu.HBM((2 * N1, 4 * N1), jnp.bfloat16),
            jax.ShapeDtypeStruct((HALF, HALF), jnp.bfloat16),
        ],
        in_specs=[VMEM],
        out_specs=[VMEM, VMEM, VMEM],
        compiler_params=KERNEL,
    )(second)
    fourth = pltpu.with_memory_space_constraint(fourth, pltpu.HBM)
    gains = pltpu.with_memory_space_constraint(skip_gain, pltpu.HBM)
    mixed = pl.pallas_call(
        convolve,
        out_shape=jax.ShapeDtypeStruct((4, 2 * N1, HALF), jnp.bfloat16),
        in_specs=[HBM] + [VMEM] * 7 + [HBM],
        out_specs=VMEM,
        scratch_shapes=[
            pltpu.SMEM((N1,), jnp.float32),
            pltpu.VMEM((2 * N1, 4 * N1), jnp.bfloat16),
            pltpu.SemaphoreType.DMA((2,)),
        ],
        compiler_params=KERNEL,
    )(gains, u, filt, order, first, second, cos_tw, sin_tw, fourth)
    mixed = mixed.reshape(4 * 64, 8, HALF)
    back = exchange(mixed)
    return back.transpose(1, 2, 0).reshape(1, 8 * HALF, channels)


def solution(mesh):
    split = Mesh(mesh.devices.reshape(2, 32, 4, 2), ("yh", "xz", "ylo", "core"))
    bat, seq = ("ylo", "core"), ("yh", "xz")
    placed = (P(bat, seq, None), P(None, seq, None, bat), P())
    return jax.shard_map(layer, mesh=split, in_specs=placed, out_specs=P(bat, seq, None), check_vma=False)
```

```python
import math

import jax
import jax.numpy as jnp
import numpy as np
from jax import lax
from jax.experimental import pallas as pl
from jax.experimental.pallas import tpu as pltpu
from jax.sharding import Mesh
from jax.sharding import PartitionSpec as P


N1 = 256
N2 = 256
HALF = 128
ROWS = 512
EVERY = ("yh", "xz", "ylo", "core")


def home(ylo, core):
    return (ylo + 2 + 4 * core) % 8


TOKEN_GROUPS = [
    [
        ((home(ylo, block) // 4 * 32 + xz) * 4 + home(ylo, block) % 4) * 2 + core
        for ylo in range(4)
        for block in range(2)
        for xz in range(32)
    ]
    for core in range(2)
]
MEET = [
    ((yh * 4 + ylo) * 2 + core, home(ylo, core) * 2 + yh)
    for yh in range(2)
    for ylo in range(4)
    for core in range(2)
]
VMEM = pl.BlockSpec(memory_space=pltpu.VMEM)
HBM = pl.BlockSpec(memory_space=pltpu.HBM)
KERNEL = pltpu.CompilerParams(vmem_limit_bytes=24 * 1024 * 1024)


def cos_sin(rows, columns, period):
    angle = (np.arange(rows)[:, None] * np.arange(columns)[None, :] % period) * (2.0 * math.pi / period)
    return np.cos(angle).astype(np.float32), np.sin(angle).astype(np.float32)


def tables():
    c, s = cos_sin(ROWS, ROWS, ROWS)
    ch, sh = cos_sin(HALF, HALF, HALF)
    inner = np.block([[ch, -sh], [sh, ch]])
    want = np.arange(HALF)
    source = (want // 4 % 16) * 8 + (want // 64) * 4 + want % 4
    order = source[:, None] == np.arange(HALF)[None, :]
    want = np.arange(N2)
    parity = np.arange(N2)[:, None] == (want % HALF * 2 + want // HALF)[None, :]
    half = [np.asarray(table, np.float32).astype(jnp.bfloat16) for table in (c, -s, inner, order, parity)]
    return [jnp.asarray(table) for table in (*half, *cos_sin(ROWS, HALF, N1 * N2))]


def dot(a, b):
    return jnp.dot(a, b, preferred_element_type=jnp.float32)


def convolve(gains_hbm, u, filt, cos_rows, sin_rows, inner, order, parity, cos_tw, sin_tw, out, gains, arrived):
    copy = pltpu.make_async_copy(gains_hbm, gains, arrived)
    copy.start()
    block = (lax.axis_index("yh") * 4 + lax.axis_index("ylo") + 6) % 8
    channel = (block % 4) * 64 + (block // 4) * 32 + lax.axis_index("xz")
    batches = u.shape[0]
    wide = jnp.concatenate([u[b] for b in range(batches)], axis=1)
    section_re, section_im = dot(cos_rows[...], wide), dot(sin_rows[...], wide)
    blocks = [dot(order[...], filt[i * HALF : (i + 1) * HALF]).astype(jnp.bfloat16) for i in range(4)]
    parts = [block[:64] for block in blocks] + [block[64:] for block in blocks]
    weights = dot(jnp.concatenate(parts, axis=0), parity[...])
    wr = jnp.concatenate([weights[:N1, :HALF], weights[:N1, HALF:]], axis=0)
    wi = jnp.concatenate([weights[N1:, :HALF], weights[N1:, HALF:]], axis=0)
    c, s = cos_tw[...], sin_tw[...]
    for first_of_two in range(0, batches, 2):
        rows_re, rows_im = [], []
        for b in (first_of_two, first_of_two + 1):
            re, im = section_re[:, b * HALF : (b + 1) * HALF], section_im[:, b * HALF : (b + 1) * HALF]
            turned = jnp.concatenate([re * c + im * s, im * c - re * s], axis=1).astype(jnp.bfloat16)
            spectrum = dot(turned, inner[...])
            sr, si = spectrum[:, :HALF], spectrum[:, HALF:]
            product = jnp.concatenate([sr * wr - si * wi, -(sr * wi) - si * wr], axis=1).astype(jnp.bfloat16)
            back = dot(product, inner[...])
            br, nbi = back[:, :HALF], back[:, HALF:]
            rows_re.append((br * c + nbi * s).astype(jnp.bfloat16))
            rows_im.append((br * s - nbi * c).astype(jnp.bfloat16))
        if first_of_two == 0:
            copy.wait()
        filtered = dot(cos_rows[...], jnp.concatenate(rows_re, axis=1))
        filtered = filtered + dot(sin_rows[...], jnp.concatenate(rows_im, axis=1))
        filtered = filtered * (1.0 / (N1 * N2))
        for i in range(2):
            b = first_of_two + i
            skip = gains[channel] * u[b].astype(jnp.float32)
            out[b] = (filtered[:, i * HALF : (i + 1) * HALF] + skip).astype(jnp.bfloat16)


def exchange(chunks):
    return lax.all_to_all(
        chunks, EVERY, split_axis=0, concat_axis=0, tiled=True, axis_index_groups=TOKEN_GROUPS
    )


def layer(tokens, filter_spectrum, skip_gain):
    channels = tokens.shape[-1]
    mine = filter_spectrum.transpose(3, 0, 1, 2).reshape(32, 8, N2)
    mine = lax.all_to_all(mine, "xz", split_axis=0, concat_axis=0, tiled=True)
    laid_out = tokens.reshape(8, HALF, channels).transpose(2, 0, 1)
    u = exchange(laid_out)
    u = u.reshape(4, ROWS, HALF)
    mine = lax.ppermute(mine, ("yh", "ylo", "core"), MEET)
    filt = lax.all_gather(mine, "core", axis=0, tiled=True)
    filt = filt.reshape(ROWS, N2)
    gains = pltpu.with_memory_space_constraint(skip_gain, pltpu.HBM)
    mixed = pl.pallas_call(
        convolve,
        out_shape=jax.ShapeDtypeStruct((4, ROWS, HALF), jnp.bfloat16),
        in_specs=[HBM] + [VMEM] * 9,
        out_specs=VMEM,
        scratch_shapes=[pltpu.SMEM((N1,), jnp.float32), pltpu.SemaphoreType.DMA],
        compiler_params=KERNEL,
    )(gains, u, filt, *tables())
    mixed = mixed.reshape(4 * 64, 8, HALF)
    back = exchange(mixed)
    return back.transpose(1, 2, 0).reshape(1, 8 * HALF, channels)


def solution(mesh):
    split = Mesh(mesh.devices.reshape(2, 32, 4, 2), ("yh", "xz", "ylo", "core"))
    bat, seq = ("ylo", "core"), ("yh", "xz")
    placed = (P(bat, seq, None), P(None, seq, None, bat), P())
    return jax.shard_map(layer, mesh=split, in_specs=placed, out_specs=P(bat, seq, None), check_vma=False)
```

```python
import math

import jax
import jax.numpy as jnp
import numpy as np
from jax import lax
from jax.experimental import pallas as pl
from jax.experimental.pallas import tpu as pltpu
from jax.sharding import Mesh
from jax.sharding import PartitionSpec as P


N1 = 256
N2 = 256
HALF = 128
ROWS = 512
EVERY = ("yh", "xz", "ylo", "core")


def home(ylo, core):
    return (ylo + 2 + 4 * core) % 8


def turn(y):
    return (10 * y + 4 * (y // 4)) % 32


def device(y, xz, core):
    return ((y // 4 * 32 + xz) * 4 + y % 4) * 2 + core


BLOCKS = [(ylo, core) for ylo in range(4) for core in range(2)]
TOKEN_GROUPS = [
    [device(home(*block), (i + turn(home(*block))) % 32, core) for block in BLOCKS for i in range(32)]
    for core in range(2)
]
FILTER_GROUPS = [
    [device(yh * 4 + ylo, (i + turn(home(ylo, core))) % 32, core) for i in range(32)]
    for yh in range(2)
    for ylo, core in BLOCKS
]
MEET = [
    ((yh * 4 + ylo) * 2 + core, home(ylo, core) * 2 + yh)
    for yh in range(2)
    for ylo in range(4)
    for core in range(2)
]
VMEM = pl.BlockSpec(memory_space=pltpu.VMEM)
HBM = pl.BlockSpec(memory_space=pltpu.HBM)
KERNEL = pltpu.CompilerParams(vmem_limit_bytes=24 * 1024 * 1024)


def cos_sin(rows, columns, period):
    angle = (np.arange(rows)[:, None] * np.arange(columns)[None, :] % period) * (2.0 * math.pi / period)
    return np.cos(angle).astype(np.float32), np.sin(angle).astype(np.float32)


def tables():
    c, s = cos_sin(ROWS, ROWS, ROWS)
    ch, sh = cos_sin(HALF, HALF, HALF)
    inner = np.block([[ch, -sh], [sh, ch]])
    want = np.arange(N2)
    parity = np.arange(N2)[:, None] == (want % HALF * 2 + want // HALF)[None, :]
    half = [np.asarray(table, np.float32).astype(jnp.bfloat16) for table in (c, -s, inner, parity)]
    return [jnp.asarray(table) for table in (*half, *cos_sin(ROWS, HALF, N1 * N2))]


def dot(a, b):
    return jnp.dot(a, b, preferred_element_type=jnp.float32)


def convolve(gains_hbm, u, filt, cos_rows, sin_rows, inner, parity, cos_tw, sin_tw, out, gains, arrived):
    copy = pltpu.make_async_copy(gains_hbm, gains, arrived)
    copy.start()
    y = lax.axis_index("yh") * 4 + lax.axis_index("ylo")
    block = (y + 6) % 8
    channel = (block % 4) * 64 + (block // 4) * 32 + (lax.axis_index("xz") + 32 - turn(y)) % 32
    batches = 4
    halves = [[((b + 4 * yh + 6) % 4 * 2 + (b + 4 * yh + 6) % 8 // 4, turn(b + 4 * yh)) for yh in range(2)] for b in range(batches)]
    tokens = []
    for pair in halves:
        tiles = []
        for slot, start in pair:
            tiles += [u[slot, 32 - start :]] if start else []
            tiles.append(u[slot, : 32 - start])
        tokens.append(jnp.concatenate([tile.reshape(-1, HALF) for tile in tiles], axis=0))
    wide = jnp.concatenate(tokens, axis=1)
    section_re, section_im = dot(cos_rows[...], wide), dot(sin_rows[...], wide)
    want = lax.broadcasted_iota(jnp.int32, (N1, N1), 0)
    source = (want // 4 + 32 - turn(y)) % 32 * 8 + want // HALF * 4 + want % 4
    order = jnp.where(source == lax.broadcasted_iota(jnp.int32, (N1, N1), 1), 1.0, 0.0).astype(jnp.bfloat16)
    blocks = [dot(order, filt[yh * N1 : (yh + 1) * N1]).astype(jnp.bfloat16) for yh in range(2)]
    parts = [block[:HALF] for block in blocks] + [block[HALF:] for block in blocks]
    weights = dot(jnp.concatenate(parts, axis=0), parity[...])
    wr = jnp.concatenate([weights[:N1, :HALF], weights[:N1, HALF:]], axis=0)
    wi = jnp.concatenate([weights[N1:, :HALF], weights[N1:, HALF:]], axis=0)
    c, s = cos_tw[...], sin_tw[...]
    for first_of_two in range(0, batches, 2):
        rows_re, rows_im = [], []
        for b in (first_of_two, first_of_two + 1):
            re, im = section_re[:, b * HALF : (b + 1) * HALF], section_im[:, b * HALF : (b + 1) * HALF]
            turned = jnp.concatenate([re * c + im * s, im * c - re * s], axis=1).astype(jnp.bfloat16)
            spectrum = dot(turned, inner[...])
            sr, si = spectrum[:, :HALF], spectrum[:, HALF:]
            product = jnp.concatenate([sr * wr - si * wi, -(sr * wi) - si * wr], axis=1).astype(jnp.bfloat16)
            back = dot(product, inner[...])
            br, nbi = back[:, :HALF], back[:, HALF:]
            rows_re.append((br * c + nbi * s).astype(jnp.bfloat16))
            rows_im.append((br * s - nbi * c).astype(jnp.bfloat16))
        if first_of_two == 0:
            copy.wait()
        filtered = dot(cos_rows[...], jnp.concatenate(rows_re, axis=1))
        filtered = filtered + dot(sin_rows[...], jnp.concatenate(rows_im, axis=1))
        filtered = filtered * (1.0 / (N1 * N2))
        for i in range(2):
            b = first_of_two + i
            skip = gains[channel] * tokens[b].astype(jnp.float32)
            mixed = (filtered[:, i * HALF : (i + 1) * HALF] + skip).astype(jnp.bfloat16)
            mixed = mixed.reshape(64, 8, HALF)
            for yh, (slot, start) in enumerate(halves[b]):
                out[slot, : 32 - start] = mixed[yh * 32 + start : yh * 32 + 32]
                if start:
                    out[slot, 32 - start :] = mixed[yh * 32 : yh * 32 + start]


def exchange(chunks):
    return lax.all_to_all(
        chunks, EVERY, split_axis=0, concat_axis=0, tiled=True, axis_index_groups=TOKEN_GROUPS
    )


def layer(tokens, filter_spectrum, skip_gain):
    channels = tokens.shape[-1]
    mine = filter_spectrum.transpose(3, 0, 1, 2).reshape(32, 8, N2)
    mine = lax.all_to_all(
        mine, EVERY, split_axis=0, concat_axis=0, tiled=True, axis_index_groups=FILTER_GROUPS
    )
    laid_out = tokens.reshape(8, HALF, channels).transpose(2, 0, 1)
    u = exchange(laid_out)
    u = u.reshape(8, 32, 8, HALF)
    mine = lax.ppermute(mine, ("yh", "ylo", "core"), MEET)
    filt = lax.all_gather(mine, "core", axis=0, tiled=True)
    filt = filt.reshape(ROWS, N2)
    gains = pltpu.with_memory_space_constraint(skip_gain, pltpu.HBM)
    mixed = pl.pallas_call(
        convolve,
        out_shape=jax.ShapeDtypeStruct((8, 32, 8, HALF), jnp.bfloat16),
        in_specs=[HBM] + [VMEM] * 8,
        out_specs=VMEM,
        scratch_shapes=[pltpu.SMEM((N1,), jnp.float32), pltpu.SemaphoreType.DMA],
        compiler_params=KERNEL,
    )(gains, u, filt, *tables())
    mixed = mixed.reshape(channels, 8, HALF)
    back = exchange(mixed)
    return back.transpose(1, 2, 0).reshape(1, 8 * HALF, channels)


def solution(mesh):
    split = Mesh(mesh.devices.reshape(2, 32, 4, 2), ("yh", "xz", "ylo", "core"))
    bat, seq = ("ylo", "core"), ("yh", "xz")
    placed = (P(bat, seq, None), P(None, seq, None, bat), P())
    return jax.shard_map(layer, mesh=split, in_specs=placed, out_specs=P(bat, seq, None), check_vma=False)
```
